256 devices in a mesh: frag: 16 (over x, y), tile: 8 (over z), ka: 2 (over core).
Axes of the slice: x: 4, y: 4, z: 8, core: 2. Of those that a mesh axis runs over, the one named last changes fastest.
Arguments:
- sizes: int32 [128], replicated, may hold values from 40 to 400
- neighbors: int32 [128, 4], P('frag'), may hold values from 0 to 127, as said below
- slot_fragment: int32 [128], replicated, may hold values from 0 to 127, as said below
- density: bfloat16 [128, 512, 512], P('frag', ('tile', 'ka')), may hold values from -6 to 6
- hcore: bfloat16 [128, 512, 512], P('frag', ('tile', 'ka')), may hold values from -3 to 3
- integrals: bfloat16 [128, 32, 512, 512], P('frag', ('tile', 'ka')), may hold values from -0.15625 to 0.15625
- couple: bfloat16 [128, 4, 512, 512], P('frag', None, ('tile', 'ka')), may hold values from -2.390625 to 2.390625
Outputs:
- fock: float32 [128, 512, 512], P('frag', ('tile', 'ka'))
The draws below stay inside these ranges and needn't reach their ends.
Inputs may be any that keep to these rules, and one draw needn't show every extreme that they name: `neighbors`: fragment f belongs to group f // 8; each entry names a fragment other than f itself, belonging to the same group or to the next group on either side. `slot_fragment`: A permutation of the fragments; slots s with s // 8 == h form balanced group h; no group's fragments fill more than 1 slots of one balanced group, and some pair of groups reaches 1.
All inputs are finite; a program needn't handle non-finite values.
Results may differ from the reference program's by a relative error of at most 0.002.
Values may be sent and summed in bfloat16 or wider, within the bound.
No kernel may reach another device: no remote copies, remote signals or barrier semaphores. Data moves between devices by JAX's collectives and lax.ppermute only.
A program may use at most 64 MiB of HBM per device.

```python
import jax
import jax.numpy as jnp
from jax import lax

TILE = 128
NB = 512
FPG = 8
NFRAG = 128
CHOL = 32
NNB = 4
N_FRAG = 16


def draw_layout(key):
    base = jax.random.fold_in(key, 11)
    keys = jax.random.split(base, 8)
    fragments = jnp.arange(NFRAG, dtype=jnp.int32)
    owner_group = fragments // FPG
    peptide = jax.random.randint(keys[0], (N_FRAG,), 0, 10) < 3
    chosen = jax.random.randint(keys[1], (), 0, N_FRAG)
    peptide = peptide | (jnp.arange(N_FRAG) == chosen)
    water_size = jax.random.randint(keys[2], (NFRAG,), TILE * 5 // 16, TILE + 1)
    peptide_size = jax.random.randint(keys[3], (NFRAG,), TILE * 3 // 2, NB * 25 // 32 + 1)
    frag_sizes = jnp.where(peptide[owner_group], peptide_size, water_size).astype(jnp.int32)
    scores = (frag_sizes * FPG + fragments % FPG).reshape(N_FRAG, FPG)
    rank_order = jnp.argsort(-scores, axis=1, stable=True).astype(jnp.int32)
    offset_perm = jax.random.permutation(keys[4], N_FRAG).astype(jnp.int32)
    offsets = offset_perm[jnp.arange(FPG) % N_FRAG]
    group_perm = jax.random.permutation(keys[5], N_FRAG).astype(jnp.int32)
    other_perm = jax.random.permutation(keys[6], N_FRAG).astype(jnp.int32)
    group_inv = jnp.argsort(group_perm).astype(jnp.int32)
    other_inv = jnp.argsort(other_perm).astype(jnp.int32)
    source = group_inv[(other_inv[:, None] - offsets[None, :]) % N_FRAG]
    ranks = jnp.broadcast_to(jnp.arange(FPG, dtype=jnp.int32)[None, :], (N_FRAG, FPG))
    placed = source * FPG + rank_order[source, ranks]
    shuffle = jax.random.randint(keys[7], (N_FRAG, FPG), 0, 1 << 20) * FPG + ranks
    slot_perm = jnp.argsort(shuffle, axis=1, stable=True).astype(jnp.int32)
    slots = jnp.take_along_axis(placed, slot_perm, axis=1).reshape(NFRAG).astype(jnp.int32)
    return (frag_sizes, slots)


def draw_sizes(key, part):
    return draw_layout(key)[0]


def draw_slot_fragment(key, part):
    return draw_layout(key)[1]


def draw_neighbors(key, part):
    base = jax.random.fold_in(key, 23)
    keys = jax.random.split(base, 3)
    fragments = jnp.arange(NFRAG, dtype=jnp.int32)
    owner_group = fragments // FPG
    group_step = jax.random.randint(keys[0], (NFRAG, NNB), -1, 2)
    near_group = owner_group[:, None] + group_step
    near_group = jnp.where(near_group < 0, 1, near_group)
    near_group = jnp.where(near_group >= N_FRAG, N_FRAG - 2, near_group)
    local_shift = jax.random.randint(keys[1], (NFRAG, NNB), 1, FPG)
    any_local = jax.random.randint(keys[2], (NFRAG, NNB), 0, FPG)
    local_index = jnp.where(near_group == owner_group[:, None], (fragments[:, None] % FPG + local_shift) % FPG, any_local)
    return (near_group * FPG + local_index).astype(jnp.int32)


def level_of(stream_key, extent, cuts, low, top_value):
    def one(dim, shards_of):
        heights = jax.random.uniform(jax.random.fold_in(jax.random.fold_in(stream_key, 6), dim), (shards_of,), jnp.float32, low / len(cuts), top_value / len(cuts))
        return jnp.repeat(jnp.exp(heights), extent[dim] // shards_of).reshape((-1,) + (1,) * (len(extent) - dim - 1))

    loudness = one(*cuts[0])
    for cut in cuts[1:]:
        loudness = loudness * one(*cut)
    return loudness


def normal_values(key, shape, width, limit, pieces=(), kind=jnp.bfloat16):
    array = jax.random.normal(key, shape, jnp.float32) * width
    if len(pieces) > 0:
        array = level_of(key, shape, pieces, -0.22, 0.18) * array
    return jnp.clip(array, min=-limit, max=limit).astype(kind)


def setup_inputs(seed: int = 0) -> dict:
    splits = jax.random.split(jax.random.key(seed), 8)
    return {
        "sizes": draw_sizes(jax.random.fold_in(splits[7], 71), 0),
        "neighbors": draw_neighbors(jax.random.fold_in(splits[7], 71), 0),
        "slot_fragment": draw_slot_fragment(jax.random.fold_in(splits[7], 71), 0),
        "density": normal_values(splits[3], (NFRAG, NB, NB), 1.0, 6.0, ((0, 16), (1, 16))),
        "hcore": normal_values(splits[4], (NFRAG, NB, NB), 0.5, 3.0, ((0, 16), (1, 16))),
        "integrals": normal_values(splits[5], (NFRAG, CHOL, NB, NB), (3 * NB) ** -0.5, 0.15625, ((0, 16), (1, 16))),
        "couple": normal_values(splits[6], (NFRAG, NNB, NB, NB), 0.4, 2.390625, ((0, 16), (2, 16))),
    }


def reference(sizes, neighbors, slot_fragment, density, hcore, integrals, couple):
    positions = jnp.arange(NB, dtype=jnp.int32)
    keep_mask = ((positions[None, :, None] < sizes[:, None, None]) & (positions[None, None, :] < sizes[:, None, None])).astype(jnp.float32)
    masked = (density.astype(jnp.float32) * keep_mask).astype(jnp.bfloat16)
    slot_of = jnp.zeros((NFRAG,), jnp.int32).at[slot_fragment].set(jnp.arange(NFRAG, dtype=jnp.int32))

    def fragment_fock(fragment):
        factors = integrals[slot_of[fragment]].astype(jnp.float32)
        frag_density = masked[fragment].astype(jnp.float32)
        product = jnp.einsum('qik,kj->qij', factors, frag_density, precision=lax.Precision.HIGHEST)
        product = product.astype(jnp.bfloat16).astype(jnp.float32)
        exchange_term = jnp.einsum('qij,qlj->qil', product, factors, precision=lax.Precision.HIGHEST)
        coulomb = jnp.einsum('qij,ij->q', factors, frag_density, precision=lax.Precision.HIGHEST)
        two_body = jnp.sum(coulomb[:, None, None] * factors - 0.5 * exchange_term, axis=0)
        picked = masked[neighbors[fragment]].astype(jnp.float32)
        coupling = jnp.sum(couple[fragment].astype(jnp.float32) * picked, axis=0)
        return keep_mask[fragment] * (hcore[fragment].astype(jnp.float32) + two_body + coupling)

    return lax.map(fragment_fock, jnp.arange(NFRAG, dtype=jnp.int32))
```

```python
import functools

import jax
import jax.numpy as jnp
from jax import lax
from jax.experimental import pallas as pl
from jax.experimental.pallas import tpu as pltpu
from jax.sharding import PartitionSpec as P

F16 = jnp.float16
F32 = jnp.float32
BF16 = jnp.bfloat16
TILE = 128
TILES = 4
CLASSES = (14, 16, 18, 22, 32)
PAIR_SCALE = 0.25
SUM_SCALE = 0.03125
SMEM = pl.BlockSpec(memory_space=pltpu.SMEM)
VMEM = pl.BlockSpec(memory_space=pltpu.VMEM)


def tiles_of(size):
    return (size + (TILE - 1)) // TILE


def held_slot(sizes, slots, first, k):
    frag = slots[first + k]
    return frag, tiles_of(sizes[frag])


def masked_rows(value, size, first_row, first_col):
    rows = first_row + lax.broadcasted_iota(jnp.int32, value.shape, 0)
    cols = first_col + lax.broadcasted_iota(jnp.int32, value.shape, 1)
    return jnp.where((rows < size) & (cols < size), value, jnp.zeros_like(value))


def send_body(where, sizes, slots, density, out, kind, pack, back, targets):
    per_group, slab, width = density.shape
    groups = out.shape[0]
    first = where[0] * per_group
    widest = jnp.int32(0)
    for group in range(groups):
        total = jnp.int32(0)
        for k in range(per_group):
            frag = slots[group * per_group + k]
            total = total + tiles_of(sizes[frag])
            local = frag - first
            inside = (local >= 0) & (local < per_group)
            targets[jnp.where(inside, local, per_group)] = group
        widest = jnp.maximum(widest, total)
    index = jnp.int32(0)
    for limit in CLASSES[:-1]:
        index = index + (widest > limit).astype(jnp.int32)
    kind[0] = index
    for place in range(pack.shape[0]):
        pack[place] = 0
    for place in range(back.shape[0]):
        back[place] = 0
    offset = jnp.int32(0)
    for k in range(per_group):
        frag, count = held_slot(sizes, slots, first, k)
        source = frag // per_group
        for c in range(TILES):
            valid = c < count
            pack[jnp.where(valid, offset + c, pack.shape[0] - 1)] = source * TILES + c
            back[source * TILES + c] = jnp.where(valid, offset + c, 0)
        offset = offset + count
    for j in range(per_group):
        rows = masked_rows(
            density[j].astype(F32), sizes[first + j], where[1] * slab, 0
        ).astype(BF16)
        for c in range(width // TILE):
            out[targets[j], c] = rows[:, c * TILE : (c + 1) * TILE]


def fock_body(where, sizes, slots, gathered, factors, keep, send, dense):
    k = pl.program_id(0)
    per_group = pl.num_programs(0)
    first = where[0] * per_group
    _, count = held_slot(sizes, slots, first, k)
    offset = jnp.int32(0)
    for other in range(8):
        _, width = held_slot(sizes, slots, first, other)
        offset = offset + jnp.where(other < k, width, 0)
    mine = where[2]
    lanes = gathered.shape[0]
    slab = gathered.shape[2]
    chol = factors.shape[1]

    def run(tiles):
        extent = tiles * TILE
        for lane in range(extent // slab):
            for c in range(tiles):
                dense[lane * slab : (lane + 1) * slab, c * TILE : (c + 1) * TILE] = (
                    gathered[lane, offset + c]
                )
        block = dense[:extent, :extent]
        total = jnp.zeros((extent, extent), F32)
        wide = block.astype(F32)
        for q in range(chol):
            factor = factors[0, q, :extent, :extent]
            long = factor.astype(F32)
            product = jnp.dot(factor, block, preferred_element_type=F32).astype(BF16)
            exchange = lax.dot_general(
                product, factor, (((1,), (1,)), ((), ())), preferred_element_type=F32
            )
            coulomb = jnp.sum(long * wide)
            total = total + (coulomb * long - 0.5 * exchange)
        for lane in range(extent // slab):
            for c in range(tiles):
                piece = total[lane * slab : (lane + 1) * slab, c * TILE : (c + 1) * TILE]

                @pl.when(mine == lane % 2)
                def _():
                    keep[lane // 2, offset + c] = piece

                @pl.when(mine != lane % 2)
                def _():
                    send[lane // 2, offset + c] = piece

    for tiles in range(1, TILES + 1):
        pl.when(count == tiles)(functools.partial(run, tiles))


def base_body(where, sizes, neighbors, low, own, high, hcore, couple, out):
    per_group, slab, _ = own.shape
    first = where[0] * per_group
    row = where[1] * slab
    for j in range(per_group):
        out[j] = hcore[j].astype(F32)
        for k in range(neighbors.shape[1]):
            near = neighbors[j, k]
            size = sizes[near]
            place = near - first
            weight = couple[j, k].astype(F32)
            side = place // per_group
            local = place - side * per_group

            def add(source):
                rows = masked_rows(source[local].astype(F32), size, row, 0)
                out[j] += weight * rows

            pl.when(side == 0)(lambda: add(own))
            pl.when(side < 0)(lambda: add(low))
            pl.when(side > 0)(lambda: add(high))


def local(sizes, neighbors, slot_fragment, density, hcore, integrals, couple):
    groups = lax.axis_size("frag")
    cores = lax.axis_size("ka")
    chips = lax.axis_size("tile")
    group = lax.axis_index("frag")
    core = lax.axis_index("ka")
    lane = lax.axis_index("tile") * cores + core
    per_group, slab, width = density.shape
    where = jnp.stack([group, lane, core]).astype(jnp.int32)
    low = lax.ppermute(density, "frag", [(i, i + 1) for i in range(groups - 1)])
    high = lax.ppermute(density, "frag", [(i + 1, i) for i in range(groups - 1)])

    block = (groups, TILES, slab, TILE)
    table = lambda count: jax.ShapeDtypeStruct((count,), jnp.int32)
    outgoing, kind, pack, back, targets = pl.pallas_call(
        send_body,
        out_shape=(
            jax.ShapeDtypeStruct(block, BF16),
            table(1),
            table(per_group * TILES + 1),
            table(groups * TILES),
            table(per_group + 1),
        ),
        in_specs=[SMEM, SMEM, SMEM, VMEM],
        out_specs=(VMEM, SMEM, SMEM, SMEM, SMEM),
        name="send",
    )(where, sizes, slot_fragment, density)
    received = lax.all_to_all(outgoing, "frag", split_axis=0, concat_axis=0, tiled=True)
    base = pl.pallas_call(
        base_body,
        out_shape=jax.ShapeDtypeStruct(density.shape, F32),
        in_specs=[SMEM] * 3 + [VMEM] * 5,
        out_specs=VMEM,
        name="base",
    )(where, sizes, neighbors, low, density, high, hcore, couple)

    def balanced(capacity, received):
        flat = received.reshape(groups * TILES, slab, TILE)
        packed = jnp.take(flat, pack[:capacity], axis=0, mode="clip").astype(F16)
        gathered = lax.all_gather(packed, ("tile", "ka"), axis=0, tiled=False).astype(BF16)
        half = jax.ShapeDtypeStruct((chips, capacity, slab, TILE), F32)
        keep, send = pl.pallas_call(
            fock_body,
            grid=(per_group,),
            out_shape=(half, half),
            in_specs=[
                SMEM,
                SMEM,
                SMEM,
                pl.BlockSpec(gathered.shape, lambda k: (0, 0, 0, 0)),
                pl.BlockSpec((1,) + integrals.shape[1:], lambda k: (k, 0, 0, 0)),
            ],
            out_specs=(
                pl.BlockSpec(half.shape, lambda k: (0, 0, 0, 0)),
                pl.BlockSpec(half.shape, lambda k: (0, 0, 0, 0)),
            ),
            scratch_shapes=[pltpu.VMEM((width, width), BF16)],
            compiler_params=pltpu.CompilerParams(dimension_semantics=("arbitrary",)),
            name="fock",
        )(where, sizes, slot_fragment, gathered, integrals)
        other = lax.ppermute(send, "ka", [(0, 1), (1, 0)])
        pair = ((keep + other) * PAIR_SCALE).astype(F16)
        parts = lax.all_to_all(pair, "tile", split_axis=0, concat_axis=0, tiled=True)
        total = jnp.sum(parts.astype(F32), axis=0)
        return jnp.take(total * (SUM_SCALE / PAIR_SCALE), back, axis=0, mode="clip").astype(F16)

    branches = [functools.partial(balanced, capacity) for capacity in CLASSES]
    summed = lax.switch(kind[0], branches, received).reshape(block)
    returned = lax.all_to_all(summed, "frag", split_axis=0, concat_axis=0, tiled=True)
    picked = jnp.take(returned, targets[:per_group], axis=0, mode="clip")
    two_body = picked.astype(F32).transpose(0, 2, 1, 3).reshape(density.shape)
    own_sizes = lax.dynamic_slice_in_dim(sizes, group * per_group, per_group)[:, None, None]
    rows = lane * slab + lax.broadcasted_iota(jnp.int32, density.shape, 1)
    cols = lax.broadcasted_iota(jnp.int32, density.shape, 2)
    keep = (rows < own_sizes) & (cols < own_sizes)
    return jnp.where(keep, base + two_body * (1.0 / SUM_SCALE), 0.0)


def solution(mesh):
    return jax.shard_map(
        local,
        mesh=mesh,
        in_specs=(
            P(),
            P("frag", None),
            P(),
            P("frag", ("tile", "ka"), None),
            P("frag", ("tile", "ka"), None),
            P("frag", ("tile", "ka"), None, None),
            P("frag", None, ("tile", "ka"), None),
        ),
        out_specs=P("frag", ("tile", "ka"), None),
        check_vma=False,
    )
```

```python
import functools

import jax
import jax.numpy as jnp
from jax import lax
from jax.experimental import pallas as pl
from jax.experimental.pallas import tpu as pltpu
from jax.sharding import PartitionSpec as P

F16 = jnp.float16
F32 = jnp.float32
BF16 = jnp.bfloat16
TILE = 128
TILES = 4
CLASSES = (16, 19, 32)
PAIR_SCALE = 0.25
SUM_SCALE = 0.03125
SMEM = pl.BlockSpec(memory_space=pltpu.SMEM)
VMEM = pl.BlockSpec(memory_space=pltpu.VMEM)


def tiles_of(size):
    return (size + (TILE - 1)) // TILE


def held_slot(sizes, slots, first, k):
    frag = slots[first + k]
    return frag, tiles_of(sizes[frag])


def masked_rows(value, size, first_row, first_col):
    rows = first_row + lax.broadcasted_iota(jnp.int32, value.shape, 0)
    cols = first_col + lax.broadcasted_iota(jnp.int32, value.shape, 1)
    return jnp.where((rows < size) & (cols < size), value, jnp.zeros_like(value))


def send_body(where, sizes, slots, density, out, kind, pack, back, targets):
    per_group, slab, width = density.shape
    groups = out.shape[0]
    first = where[0] * per_group
    widest = jnp.int32(0)
    for group in range(groups):
        total = jnp.int32(0)
        for k in range(per_group):
            frag = slots[group * per_group + k]
            total = total + tiles_of(sizes[frag])
            local = frag - first
            inside = (local >= 0) & (local < per_group)
            targets[jnp.where(inside, local, per_group)] = group
        widest = jnp.maximum(widest, total)
    index = jnp.int32(0)
    for limit in CLASSES[:-1]:
        index = index + (widest > limit).astype(jnp.int32)
    kind[0] = index
    for place in range(pack.shape[0]):
        pack[place] = 0
    for place in range(back.shape[0]):
        back[place] = 0
    offset = jnp.int32(0)
    for k in range(per_group):
        frag, count = held_slot(sizes, slots, first, k)
        source = frag // per_group
        for c in range(TILES):
            valid = c < count
            pack[jnp.where(valid, offset + c, pack.shape[0] - 1)] = source * TILES + c
            back[source * TILES + c] = jnp.where(valid, offset + c, 0)
        offset = offset + count
    for j in range(per_group):
        rows = masked_rows(
            density[j].astype(F32), sizes[first + j], where[1] * slab, 0
        ).astype(BF16)
        for c in range(width // TILE):
            out[targets[j], c] = rows[:, c * TILE : (c + 1) * TILE]


def fock_body(
    where, sizes, slots, gathered, factors, keep, send, dense, total, *, per_group
):
    k = pl.program_id(0)
    first = where[0] * per_group
    _, count = held_slot(sizes, slots, first, k)
    offset = jnp.int32(0)
    for other in range(per_group):
        _, width = held_slot(sizes, slots, first, other)
        offset = offset + jnp.where(other < k, width, 0)
    chip = where[3]
    chips, capacity = keep.shape[:2]
    mine = where[2]
    slab = gathered.shape[2]
    chol = factors.shape[1]
    right = (chip + 1) % chips
    left = (chip + chips - 1) % chips
    half = chips // 2

    def run(tiles):
        extent = tiles * TILE

        def unpack(lane, carry):
            for c in range(tiles):
                dense[pl.ds(lane * slab, slab), c * TILE : (c + 1) * TILE] = gathered[
                    lane, offset + c
                ]
            return carry

        lax.fori_loop(0, extent // slab, unpack, 0)
        total[:extent, :extent] = jnp.zeros((extent, extent), F32)

        def vector(q, carry):
            block = dense[:extent, :extent]
            factor = factors[0, q, :extent, :extent]
            long = factor.astype(F32)
            product = jnp.dot(factor, block, preferred_element_type=F32).astype(BF16)
            exchange = lax.dot_general(
                product, factor, (((1,), (1,)), ((), ())), preferred_element_type=F32
            )
            coulomb = jnp.sum(long * block.astype(F32))
            total[:extent, :extent] += coulomb * long - 0.5 * exchange
            return carry

        lax.fori_loop(0, chol, vector, 0)

        def store(lane, carry):
            target = lane // 2
            same = (target + chip) % 2 == 0
            for c in range(tiles):
                piece = total[pl.ds(lane * slab, slab), c * TILE : (c + 1) * TILE]
                place = offset + c
                near = jnp.where(place < (capacity + 1) // 2, right, left)
                row = jnp.where(
                    same,
                    (target // 2 + half - chip // 2) % half,
                    half + (target // 2 + half - near // 2) % half,
                )

                @pl.when(mine == lane % 2)
                def _():
                    keep[row, place] = piece

                @pl.when(mine != lane % 2)
                def _():
                    send[row, place] = piece

            return carry

        lax.fori_loop(0, extent // slab, store, 0)

    for tiles in range(1, TILES + 1):
        pl.when(count == tiles)(functools.partial(run, tiles))


def base_body(where, sizes, neighbors, low, own, high, hcore, couple, out):
    per_group, slab, _ = own.shape
    first = where[0] * per_group
    row = where[1] * slab
    listed = neighbors.shape[1]

    def fragment(j, carry):
        out[j] = hcore[j].astype(F32)
        for k in range(listed):
            near = neighbors[j, k]
            size = sizes[near]
            weight = couple[j, k].astype(F32)
            place = near - first
            group = jnp.where(place < 0, 0, jnp.where(place < per_group, 1, 2))
            position = place - (group - 1) * per_group

            def add(source):
                rows = masked_rows(source[position].astype(F32), size, row, 0)
                out[j] += weight * rows

            for side, source in enumerate((low, own, high)):
                pl.when(group == side)(functools.partial(add, source))
        return carry

    lax.fori_loop(0, per_group, fragment, 0)


def local(sizes, neighbors, slot_fragment, density, hcore, integrals, couple):
    groups = lax.axis_size("frag")
    cores = lax.axis_size("ka")
    chips = lax.axis_size("tile")
    group = lax.axis_index("frag")
    core = lax.axis_index("ka")
    lane = lax.axis_index("tile") * cores + core
    per_group, slab, width = density.shape
    where = jnp.stack([group, lane, core, lax.axis_index("tile")]).astype(jnp.int32)
    shift = lambda value, by: lax.ppermute(
        value, "tile", [(i, (i + by) % chips) for i in range(chips)]
    )

    block = (groups, TILES, slab, TILE)
    table = lambda count: jax.ShapeDtypeStruct((count,), jnp.int32)
    outgoing, kind, pack, back, targets = pl.pallas_call(
        send_body,
        out_shape=(
            jax.ShapeDtypeStruct(block, BF16),
            table(1),
            table(per_group * TILES + 1),
            table(groups * TILES),
            table(per_group + 1),
        ),
        in_specs=[SMEM, SMEM, SMEM, VMEM],
        out_specs=(VMEM, SMEM, SMEM, SMEM, SMEM),
        name="send",
    )(where, sizes, slot_fragment, density)
    received = lax.all_to_all(outgoing, "frag", split_axis=0, concat_axis=0, tiled=True)
    def balanced(capacity, received):
        split = (capacity + 1) // 2
        half_chips = chips // 2
        flat = received.reshape(groups * TILES, slab, TILE)
        packed = jnp.take(flat, pack[:capacity], axis=0, mode="clip").astype(F16)
        gathered = lax.all_gather(packed, ("tile", "ka"), axis=0, tiled=False).astype(BF16)
        half = jax.ShapeDtypeStruct((chips, capacity, slab, TILE), F32)
        keep, send = pl.pallas_call(
            functools.partial(fock_body, per_group=per_group),
            grid=(per_group,),
            out_shape=(half, half),
            in_specs=[
                SMEM,
                SMEM,
                SMEM,
                pl.BlockSpec(gathered.shape, lambda k: (0, 0, 0, 0)),
                pl.BlockSpec((1,) + integrals.shape[1:], lambda k: (k, 0, 0, 0)),
            ],
            out_specs=(
                pl.BlockSpec(half.shape, lambda k: (0, 0, 0, 0)),
                pl.BlockSpec(half.shape, lambda k: (0, 0, 0, 0)),
            ),
            scratch_shapes=[pltpu.VMEM((width, width), BF16), pltpu.VMEM((width, width), F32)],
            compiler_params=pltpu.CompilerParams(dimension_semantics=("arbitrary",)),
            name="fock",
        )(where, sizes, slot_fragment, gathered, integrals)
        other = lax.ppermute(send, "ka", [(0, 1), (1, 0)])
        pair = (keep + other) * PAIR_SCALE
        up = shift(pair[half_chips:, :split].astype(F16), 1)
        down = shift(pair[half_chips:, split:].astype(F16), -1)
        own = pair[:half_chips] + jnp.concatenate([up, down], axis=1).astype(F32)
        far = own.astype(F16)
        moved = [shift(far[step], 2 * step) for step in range(1, half_chips)]
        low = lax.ppermute(density, "frag", [(i, i + 1) for i in range(groups - 1)])
        high = lax.ppermute(density, "frag", [(i + 1, i) for i in range(groups - 1)])
        base = pl.pallas_call(
            base_body,
            out_shape=jax.ShapeDtypeStruct(density.shape, F32),
            in_specs=[SMEM] * 3 + [VMEM] * 5,
            out_specs=VMEM,
            name="base",
        )(where, sizes, neighbors, low, density, high, hcore, couple)
        total = own[0] + sum(part.astype(F32) for part in moved)
        total = lax.optimization_barrier((total * (SUM_SCALE / PAIR_SCALE)).astype(F16))
        return jnp.take(total, back, axis=0, mode="clip"), base

    branches = [functools.partial(balanced, capacity) for capacity in CLASSES]
    summed, base = lax.switch(kind[0], branches, received)
    summed = summed.reshape(block)
    returned = lax.all_to_all(summed, "frag", split_axis=0, concat_axis=0, tiled=True)
    picked = jnp.take(returned, targets[:per_group], axis=0, mode="clip")
    two_body = picked.astype(F32).transpose(0, 2, 1, 3).reshape(density.shape)
    own_sizes = lax.dynamic_slice_in_dim(sizes, group * per_group, per_group)[:, None, None]
    rows = lane * slab + lax.broadcasted_iota(jnp.int32, density.shape, 1)
    cols = lax.broadcasted_iota(jnp.int32, density.shape, 2)
    keep = (rows < own_sizes) & (cols < own_sizes)
    return jnp.where(keep, base + two_body * (1.0 / SUM_SCALE), 0.0)


def solution(mesh):
    return jax.shard_map(
        local,
        mesh=mesh,
        in_specs=(
            P(),
            P("frag", None),
            P(),
            P("frag", ("tile", "ka"), None),
            P("frag", ("tile", "ka"), None),
            P("frag", ("tile", "ka"), None, None),
            P("frag", None, ("tile", "ka"), None),
        ),
        out_specs=P("frag", ("tile", "ka"), None),
        check_vma=False,
    )
```

```python
import functools

import jax
import jax.numpy as jnp
from jax import lax
from jax.experimental import pallas as pl
from jax.experimental.pallas import tpu as pltpu
from jax.sharding import PartitionSpec as P


F16 = jnp.float16
F32 = jnp.float32
BF16 = jnp.bfloat16
TILE = 128
TILES = 4
CLASSES = (16, 19, 32)
PAIR_SCALE = 0.25
SUM_SCALE = 0.03125
SMEM = pl.BlockSpec(memory_space=pltpu.SMEM)
VMEM = pl.BlockSpec(memory_space=pltpu.VMEM)


def tiles_of(size):
    return (size + (TILE - 1)) // TILE


def held_slot(sizes, slots, first, k):
    frag = slots[first + k]
    return frag, tiles_of(sizes[frag])


def masked_rows(value, size, first_row, first_col):
    rows = first_row + lax.broadcasted_iota(jnp.int32, value.shape, 0)
    cols = first_col + lax.broadcasted_iota(jnp.int32, value.shape, 1)
    return jnp.where((rows < size) & (cols < size), value, jnp.zeros_like(value))


def send_body(where, sizes, slots, density, out, kind, pack, back, targets):
    per_group, slab, width = density.shape
    groups = out.shape[0]
    first = where[0] * per_group
    widest = jnp.int32(0)
    for group in range(groups):
        total = jnp.int32(0)
        for k in range(per_group):
            frag = slots[group * per_group + k]
            total = total + tiles_of(sizes[frag])
            local = frag - first
            inside = (local >= 0) & (local < per_group)
            targets[jnp.where(inside, local, per_group)] = group
        widest = jnp.maximum(widest, total)
    index = jnp.int32(0)
    for limit in CLASSES[:-1]:
        index = index + (widest > limit).astype(jnp.int32)
    kind[0] = index
    for place in range(pack.shape[0]):
        pack[place] = 0
    for place in range(back.shape[0]):
        back[place] = 0
    offset = jnp.int32(0)
    for k in range(per_group):
        frag, count = held_slot(sizes, slots, first, k)
        source = frag // per_group
        for c in range(TILES):
            valid = c < count
            pack[jnp.where(valid, offset + c, pack.shape[0] - 1)] = source * TILES + c
            back[source * TILES + c] = jnp.where(valid, offset + c, 0)
        offset = offset + count
    for j in range(per_group):
        rows = masked_rows(
            density[j].astype(F32), sizes[first + j], where[1] * slab, 0
        ).astype(BF16)
        for c in range(width // TILE):
            out[targets[j], c] = rows[:, c * TILE : (c + 1) * TILE]


def fock_body(
    where, sizes, slots, gathered, factors, keep, send, vectors, dense, halved, total, arrived
):
    per_group = factors.shape[0]
    first = where[0] * per_group
    chip = where[3]
    chips, capacity = keep.shape[:2]
    mine = where[2]
    slab = gathered.shape[2]
    chol = factors.shape[1]
    right = (chip + 1) % chips
    left = (chip + chips - 1) % chips
    half = chips // 2

    def copies(k, tiles):
        extent = tiles * TILE
        used = pl.ds(0, extent)
        return [
            pltpu.make_async_copy(
                factors.at[k, q, used, used],
                vectors.at[k, used, pl.ds(q * extent, extent)],
                arrived.at[k, q],
            )
            for q in range(chol)
        ]

    def run(k, offset, tiles):
        extent = tiles * TILE
        pieces = [(r, c) for r in range(extent // slab) for c in range(tiles)]
        rows = lambda r: slice(r * slab, (r + 1) * slab)
        cols = lambda c: slice(c * TILE, (c + 1) * TILE)
        for r, c in pieces:
            dense[rows(r), cols(c)] = gathered[r, offset + c]
        for copy in copies(k, tiles):
            copy.wait()
        block = dense[:extent, :extent]
        for q in range(chol):
            span = slice(q * extent, (q + 1) * extent)
            product = jnp.dot(vectors[k, :extent, span], block, preferred_element_type=F32)
            halved[:extent, span] = (-0.5 * product).astype(BF16)
        wide = slice(0, chol * extent)
        total[:extent, :extent] = lax.dot_general(
            halved[:extent, wide],
            vectors[k, :extent, wide],
            (((1,), (1,)), ((), ())),
            preferred_element_type=F32,
        )
        factor = lambda q, r, c: vectors[k, rows(r), cols(q * tiles + c)].astype(F32)
        sums = [jnp.zeros((slab, TILE), F32) for _ in range(chol)]
        for r, c in pieces:
            part = dense[rows(r), cols(c)].astype(F32)
            sums = [value + factor(q, r, c) * part for q, value in enumerate(sums)]
        coulomb = [jnp.sum(value, keepdims=True) for value in sums]

        def finish(r, c):
            value = total[rows(r), cols(c)]
            for q in range(chol):
                value = value + coulomb[q] * factor(q, r, c)
            return value

        first_core = mine == 0
        for target in range(extent // (2 * slab)):
            same = (target + chip) % 2 == 0
            own_row = (target // 2 + half - chip // 2) % half
            up_row = half + (target // 2 + half - right // 2) % half
            down_row = half + (target // 2 + half - left // 2) % half
            for c in range(tiles):
                place = offset + c
                far_row = jnp.where(place < (capacity + 1) // 2, up_row, down_row)
                row = jnp.where(same, own_row, far_row)
                even = finish(2 * target, c)
                odd = finish(2 * target + 1, c)
                keep[row, place] = jnp.where(first_core, even, odd)
                send[row, place] = jnp.where(first_core, odd, even)

    for k in range(per_group):
        _, count = held_slot(sizes, slots, first, k)
        for tiles in range(1, TILES + 1):
            pl.when(count == tiles)(lambda: [copy.start() for copy in copies(k, tiles)] and None)

    def slot(k, offset):
        _, count = held_slot(sizes, slots, first, k)
        for tiles in range(1, TILES + 1):
            pl.when(count == tiles)(functools.partial(run, k, offset, tiles))
        return offset + count

    lax.fori_loop(0, per_group, slot, jnp.int32(0))


def base_body(where, sizes, neighbors, low, own, high, hcore, couple, out):
    per_group, slab, _ = own.shape
    first = where[0] * per_group
    row = where[1] * slab
    listed = neighbors.shape[1]

    def fragment(j, carry):
        out[j] = hcore[j].astype(F32)
        for k in range(listed):
            near = neighbors[j, k]
            size = sizes[near]
            weight = couple[j, k].astype(F32)
            place = near - first
            group = jnp.where(place < 0, 0, jnp.where(place < per_group, 1, 2))
            position = place - (group - 1) * per_group

            def add(source):
                rows = masked_rows(source[position].astype(F32), size, row, 0)
                out[j] += weight * rows

            for side, source in enumerate((low, own, high)):
                pl.when(group == side)(functools.partial(add, source))
        return carry

    lax.fori_loop(0, per_group, fragment, 0)


def local(sizes, neighbors, slot_fragment, density, hcore, integrals, couple):
    groups = lax.axis_size("frag")
    cores = lax.axis_size("ka")
    chips = lax.axis_size("tile")
    group = lax.axis_index("frag")
    core = lax.axis_index("ka")
    lane = lax.axis_index("tile") * cores + core
    per_group, slab, width = density.shape
    chol = integrals.shape[1]
    where = jnp.stack([group, lane, core, lax.axis_index("tile")]).astype(jnp.int32)
    shift = lambda value, by: lax.ppermute(
        value, "tile", [(i, (i + by) % chips) for i in range(chips)]
    )

    block = (groups, TILES, slab, TILE)
    table = lambda count: jax.ShapeDtypeStruct((count,), jnp.int32)
    outgoing, kind, pack, back, targets = pl.pallas_call(
        send_body,
        out_shape=(
            jax.ShapeDtypeStruct(block, BF16),
            table(1),
            table(per_group * TILES + 1),
            table(groups * TILES),
            table(per_group + 1),
        ),
        in_specs=[SMEM, SMEM, SMEM, VMEM],
        out_specs=(VMEM, SMEM, SMEM, SMEM, SMEM),
        name="send",
    )(where, sizes, slot_fragment, density)
    received = lax.all_to_all(outgoing, "frag", split_axis=0, concat_axis=0, tiled=True)

    def balanced(capacity, received):
        split = (capacity + 1) // 2
        half_chips = chips // 2
        flat = received.reshape(groups * TILES, slab, TILE)
        packed = jnp.take(flat, pack[:capacity], axis=0, mode="clip").astype(F16)
        gathered = lax.all_gather(packed, ("tile", "ka"), axis=0, tiled=False).astype(BF16)
        half = jax.ShapeDtypeStruct((chips, capacity, slab, TILE), F32)
        keep, send = pl.pallas_call(
            fock_body,
            out_shape=(half, half),
            in_specs=[SMEM] * 3 + [VMEM, pl.BlockSpec(memory_space=pl.ANY)],
            out_specs=(VMEM, VMEM),
            scratch_shapes=[
                pltpu.VMEM((per_group, width, chol * width), BF16),
                pltpu.VMEM((width, width), BF16),
                pltpu.VMEM((width, chol * width), BF16),
                pltpu.VMEM((width, width), F32),
                pltpu.SemaphoreType.DMA((per_group, chol)),
            ],
            compiler_params=pltpu.CompilerParams(
                vmem_limit_bytes=(20 + capacity // 2) << 20
            ),
            name="fock",
        )(where, sizes, slot_fragment, gathered, integrals)
        other = lax.ppermute(send, "ka", [(0, 1), (1, 0)])
        pair = (keep + other) * PAIR_SCALE
        up = shift(pair[half_chips:, :split].astype(F16), 1)
        down = shift(pair[half_chips:, split:].astype(F16), -1)
        own = pair[:half_chips] + jnp.concatenate([up, down], axis=1).astype(F32)
        far = own.astype(F16)
        slab_rows, far = lax.optimization_barrier((density, far))
        moved = [shift(far[step], 2 * step) for step in range(1, half_chips)]
        low = lax.ppermute(slab_rows, "frag", [(i, i + 1) for i in range(groups - 1)])
        high = lax.ppermute(slab_rows, "frag", [(i + 1, i) for i in range(groups - 1)])
        total = own[0] + sum(part.astype(F32) for part in moved)
        total = lax.optimization_barrier((total * (SUM_SCALE / PAIR_SCALE)).astype(F16))
        return jnp.take(total, back, axis=0, mode="clip"), low, high

    branches = [functools.partial(balanced, capacity) for capacity in CLASSES]
    summed, low, high = lax.switch(kind[0], branches, received)
    summed = summed.reshape(block)
    returned = lax.all_to_all(summed, "frag", split_axis=0, concat_axis=0, tiled=True)
    base = pl.pallas_call(
        base_body,
        out_shape=jax.ShapeDtypeStruct(density.shape, F32),
        in_specs=[SMEM] * 3 + [VMEM] * 5,
        out_specs=VMEM,
        name="base",
    )(where, sizes, neighbors, low, density, high, hcore, couple)
    picked = jnp.take(returned, targets[:per_group], axis=0, mode="clip")
    two_body = picked.astype(F32).transpose(0, 2, 1, 3).reshape(density.shape)
    own_sizes = lax.dynamic_slice_in_dim(sizes, group * per_group, per_group)[:, None, None]
    rows = lane * slab + lax.broadcasted_iota(jnp.int32, density.shape, 1)
    cols = lax.broadcasted_iota(jnp.int32, density.shape, 2)
    keep = (rows < own_sizes) & (cols < own_sizes)
    return jnp.where(keep, base + two_body * (1.0 / SUM_SCALE), 0.0)


def solution(mesh):
    return jax.shard_map(
        local,
        mesh=mesh,
        in_specs=(
            P(),
            P("frag", None),
            P(),
            P("frag", ("tile", "ka"), None),
            P("frag", ("tile", "ka"), None),
            P("frag", ("tile", "ka"), None, None),
            P("frag", None, ("tile", "ka"), None),
        ),
        out_specs=P("frag", ("tile", "ka"), None),
        check_vma=False,
    )
```

```python
import functools

import jax
import jax.numpy as jnp
from jax import lax
from jax.experimental import pallas as pl
from jax.experimental.pallas import tpu as pltpu
from jax.sharding import PartitionSpec as P


F16 = jnp.float16
F32 = jnp.float32
BF16 = jnp.bfloat16
TILE = 128
TILES = 4
CLASSES = (16, 19, 32)
PAIR_SCALE = 0.25
SUM_SCALE = 0.03125
SMALL_GRANT = 8 << 20
SMEM = pl.BlockSpec(memory_space=pltpu.SMEM)
VMEM = pl.BlockSpec(memory_space=pltpu.VMEM)


def tiles_of(size):
    return (size + (TILE - 1)) // TILE


def held_slot(sizes, slots, first, k):
    frag = slots[first + k]
    return frag, tiles_of(sizes[frag])


def masked_rows(value, size, first_row, first_col):
    rows = first_row + lax.broadcasted_iota(jnp.int32, value.shape, 0)
    cols = first_col + lax.broadcasted_iota(jnp.int32, value.shape, 1)
    return jnp.where((rows < size) & (cols < size), value, jnp.zeros_like(value))


def send_body(where, sizes, slots, density, out, targets):
    per_group, slab, width = density.shape
    first = where[0] * per_group
    for slot in range(slots.shape[0]):
        local = slots[slot] - first
        inside = (local >= 0) & (local < per_group)
        targets[jnp.where(inside, local, per_group)] = slot // per_group
    for j in range(per_group):
        rows = masked_rows(
            density[j].astype(F32), sizes[first + j], where[1] * slab, 0
        ).astype(BF16)
        for c in range(width // TILE):
            out[targets[j], c] = rows[:, c * TILE : (c + 1) * TILE]


def tables_body(where, sizes, slots, kind, pack, back):
    groups = back.shape[0] // TILES
    per_group = slots.shape[0] // groups
    first = where[0] * per_group
    widest = jnp.int32(0)
    for group in range(groups):
        total = jnp.int32(0)
        for k in range(per_group):
            total = total + held_slot(sizes, slots, group * per_group, k)[1]
        widest = jnp.maximum(widest, total)
    index = jnp.int32(0)
    for limit in CLASSES[:-1]:
        index = index + (widest > limit).astype(jnp.int32)
    kind[0] = index
    for place in range(pack.shape[0]):
        pack[place] = 0
    for place in range(back.shape[0]):
        back[place] = 0
    offset = jnp.int32(0)
    for k in range(per_group):
        frag, count = held_slot(sizes, slots, first, k)
        source = frag // per_group
        for c in range(TILES):
            valid = c < count
            pack[jnp.where(valid, offset + c, pack.shape[0] - 1)] = source * TILES + c
            back[source * TILES + c] = jnp.where(valid, offset + c, 0)
        offset = offset + count


def fock_body(
    where, sizes, slots, gathered, factors, keep, send, vectors, dense, halved, total, arrived
):
    per_group = factors.shape[0]
    first = where[0] * per_group
    chip = where[3]
    chips, capacity = keep.shape[:2]
    mine = where[2]
    slab = gathered.shape[2]
    chol = factors.shape[1]
    right = (chip + 1) % chips
    left = (chip + chips - 1) % chips
    half = chips // 2

    def copies(k, tiles):
        extent = tiles * TILE
        used = pl.ds(0, extent)
        return [
            pltpu.make_async_copy(
                factors.at[k, q, used, used],
                vectors.at[k, used, pl.ds(q * extent, extent)],
                arrived.at[k, q],
            )
            for q in range(chol)
        ]

    def run(k, offset, tiles):
        extent = tiles * TILE
        pieces = [(r, c) for r in range(extent // slab) for c in range(tiles)]
        rows = lambda r: slice(r * slab, (r + 1) * slab)
        cols = lambda c: slice(c * TILE, (c + 1) * TILE)
        for r, c in pieces:
            dense[rows(r), cols(c)] = gathered[r, offset + c]
        for copy in copies(k, tiles):
            copy.wait()
        block = dense[:extent, :extent]
        for q in range(chol):
            span = slice(q * extent, (q + 1) * extent)
            product = jnp.dot(vectors[k, :extent, span], block, preferred_element_type=F32)
            halved[:extent, span] = (-0.5 * product).astype(BF16)
        wide = slice(0, chol * extent)
        total[:extent, :extent] = lax.dot_general(
            halved[:extent, wide],
            vectors[k, :extent, wide],
            (((1,), (1,)), ((), ())),
            preferred_element_type=F32,
        )
        factor = lambda q, r, c: vectors[k, rows(r), cols(q * tiles + c)].astype(F32)
        sums = [jnp.zeros((slab, TILE), F32) for _ in range(chol)]
        for r, c in pieces:
            part = dense[rows(r), cols(c)].astype(F32)
            sums = [value + factor(q, r, c) * part for q, value in enumerate(sums)]
        coulomb = [jnp.sum(value, keepdims=True) for value in sums]

        def finish(r, c):
            value = total[rows(r), cols(c)]
            for q in range(chol):
                value = value + coulomb[q] * factor(q, r, c)
            return value

        first_core = mine == 0
        for target in range(extent // (2 * slab)):
            same = (target + chip) % 2 == 0
            own_row = (target // 2 + half - chip // 2) % half
            up_row = half + (target // 2 + half - right // 2) % half
            down_row = half + (target // 2 + half - left // 2) % half
            for c in range(tiles):
                place = offset + c
                far_row = jnp.where(place < (capacity + 1) // 2, up_row, down_row)
                row = jnp.where(same, own_row, far_row)
                even = finish(2 * target, c)
                odd = finish(2 * target + 1, c)
                keep[row, place] = jnp.where(first_core, even, odd)
                send[row, place] = jnp.where(first_core, odd, even)

    for k in range(per_group):
        _, count = held_slot(sizes, slots, first, k)
        for tiles in range(1, TILES + 1):
            pl.when(count == tiles)(lambda: [copy.start() for copy in copies(k, tiles)] and None)

    def slot(k, offset):
        _, count = held_slot(sizes, slots, first, k)
        for tiles in range(1, TILES + 1):
            pl.when(count == tiles)(functools.partial(run, k, offset, tiles))
        return offset + count

    lax.fori_loop(0, per_group, slot, jnp.int32(0))


def base_body(where, sizes, neighbors, low, own, high, hcore, couple, out):
    per_group, slab, _ = own.shape
    first = where[0] * per_group
    row = where[1] * slab
    listed = neighbors.shape[1]

    def fragment(j, carry):
        out[j] = hcore[j].astype(F32)
        for k in range(listed):
            near = neighbors[j, k]
            size = sizes[near]
            weight = couple[j, k].astype(F32)
            place = near - first
            group = jnp.where(place < 0, 0, jnp.where(place < per_group, 1, 2))
            position = place - (group - 1) * per_group

            def add(source):
                rows = masked_rows(source[position].astype(F32), size, row, 0)
                out[j] += weight * rows

            for side, source in enumerate((low, own, high)):
                pl.when(group == side)(functools.partial(add, source))
        return carry

    lax.fori_loop(0, per_group, fragment, 0)


def local(sizes, neighbors, slot_fragment, density, hcore, integrals, couple):
    groups = lax.axis_size("frag")
    cores = lax.axis_size("ka")
    chips = lax.axis_size("tile")
    group = lax.axis_index("frag")
    core = lax.axis_index("ka")
    lane = lax.axis_index("tile") * cores + core
    per_group, slab, width = density.shape
    chol = integrals.shape[1]
    where = jnp.stack([group, lane, core, lax.axis_index("tile")]).astype(jnp.int32)
    shift = lambda value, by: lax.ppermute(
        value, "tile", [(i, (i + by) % chips) for i in range(chips)]
    )

    block = (groups, TILES, slab, TILE)
    table = lambda count: jax.ShapeDtypeStruct((count,), jnp.int32)
    outgoing, targets = pl.pallas_call(
        send_body,
        out_shape=(jax.ShapeDtypeStruct(block, BF16), table(per_group + 1)),
        in_specs=[SMEM, SMEM, SMEM, VMEM],
        out_specs=(VMEM, SMEM),
        compiler_params=pltpu.CompilerParams(vmem_limit_bytes=SMALL_GRANT),
        name="send",
    )(where, sizes, slot_fragment, density)
    received = lax.all_to_all(outgoing, "frag", split_axis=0, concat_axis=0, tiled=True)
    low = lax.ppermute(density, "frag", [(i, i + 1) for i in range(groups - 1)])
    high = lax.ppermute(density, "frag", [(i + 1, i) for i in range(groups - 1)])
    kind, pack, back = pl.pallas_call(
        tables_body,
        out_shape=(table(1), table(per_group * TILES + 1), table(groups * TILES)),
        in_specs=[SMEM] * 3,
        out_specs=(SMEM, SMEM, SMEM),
        name="tables",
    )(where, sizes, slot_fragment)
    received, low, high = lax.optimization_barrier((received, low, high))

    def balanced(capacity, received):
        split = (capacity + 1) // 2
        half_chips = chips // 2
        flat = received.reshape(groups * TILES, slab, TILE)
        packed = jnp.take(flat, pack[:capacity], axis=0, mode="clip").astype(F16)
        gathered = lax.all_gather(packed, ("tile", "ka"), axis=0, tiled=False).astype(BF16)
        half = jax.ShapeDtypeStruct((chips, capacity, slab, TILE), F32)
        keep, send = pl.pallas_call(
            fock_body,
            out_shape=(half, half),
            in_specs=[SMEM] * 3 + [VMEM, pl.BlockSpec(memory_space=pl.ANY)],
            out_specs=(VMEM, VMEM),
            scratch_shapes=[
                pltpu.VMEM((per_group, width, chol * width), BF16),
                pltpu.VMEM((width, width), BF16),
                pltpu.VMEM((width, chol * width), BF16),
                pltpu.VMEM((width, width), F32),
                pltpu.SemaphoreType.DMA((per_group, chol)),
            ],
            compiler_params=pltpu.CompilerParams(
                vmem_limit_bytes=(20 + capacity // 2) << 20
            ),
            name="fock",
        )(where, sizes, slot_fragment, gathered, integrals)
        narrow = lambda value: (value * PAIR_SCALE).astype(F16)
        across = lambda value: lax.ppermute(value, "ka", [(0, 1), (1, 0)])
        far = slice(half_chips, chips)
        opposite = (keep[far] * PAIR_SCALE + across(narrow(send[far])).astype(F32)).astype(F16)
        up = shift(opposite[:, :split], 1)
        down = shift(opposite[:, split:], -1)
        near = slice(0, half_chips)
        pair = keep[near] * PAIR_SCALE + across(narrow(send[near])).astype(F32)
        own = pair + jnp.concatenate([up, down], axis=1).astype(F32)
        moved = [shift(own[step].astype(F16), 2 * step) for step in range(1, half_chips)]
        total = own[0] + sum(part.astype(F32) for part in moved)
        total = lax.optimization_barrier((total * (SUM_SCALE / PAIR_SCALE)).astype(F16))
        return jnp.take(total, back, axis=0, mode="clip")

    branches = [functools.partial(balanced, capacity) for capacity in CLASSES]
    summed = lax.switch(kind[0], branches, received)
    summed = summed.reshape(block)
    returned = lax.all_to_all(summed, "frag", split_axis=0, concat_axis=0, tiled=True)
    base = pl.pallas_call(
        base_body,
        out_shape=jax.ShapeDtypeStruct(density.shape, F32),
        in_specs=[SMEM] * 3 + [VMEM] * 5,
        out_specs=VMEM,
        compiler_params=pltpu.CompilerParams(vmem_limit_bytes=SMALL_GRANT),
        name="base",
    )(where, sizes, neighbors, low, density, high, hcore, couple)
    picked = jnp.take(returned, targets[:per_group], axis=0, mode="clip")
    two_body = picked.astype(F32).transpose(0, 2, 1, 3).reshape(density.shape)
    own_sizes = lax.dynamic_slice_in_dim(sizes, group * per_group, per_group)[:, None, None]
    rows = lane * slab + lax.broadcasted_iota(jnp.int32, density.shape, 1)
    cols = lax.broadcasted_iota(jnp.int32, density.shape, 2)
    keep = (rows < own_sizes) & (cols < own_sizes)
    return jnp.where(keep, base + two_body * (1.0 / SUM_SCALE), 0.0)


def solution(mesh):
    return jax.shard_map(
        local,
        mesh=mesh,
        in_specs=(
            P(),
            P("frag", None),
            P(),
            P("frag", ("tile", "ka"), None),
            P("frag", ("tile", "ka"), None),
            P("frag", ("tile", "ka"), None, None),
            P("frag", None, ("tile", "ka"), None),
        ),
        out_specs=P("frag", ("tile", "ka"), None),
        check_vma=False,
    )
```

```python
import functools

import jax
import jax.numpy as jnp
from jax import lax
from jax.experimental import pallas as pl
from jax.experimental.pallas import tpu as pltpu
from jax.sharding import PartitionSpec as P


F16 = jnp.float16
F32 = jnp.float32
BF16 = jnp.bfloat16
TILE = 128
TILES = 4
CLASSES = (17, 21, 32)
PAIR_SCALE = 0.25
SUM_SCALE = 0.03125
SMALL_GRANT = 8 << 20
SMEM = pl.BlockSpec(memory_space=pltpu.SMEM)
VMEM = pl.BlockSpec(memory_space=pltpu.VMEM)


def tiles_of(size):
    return (size + (TILE - 1)) // TILE


def held_slot(sizes, slots, first, k):
    frag = slots[first + k]
    return frag, tiles_of(sizes[frag])


def masked_rows(value, size, first_row, first_col):
    rows = first_row + lax.broadcasted_iota(jnp.int32, value.shape, 0)
    cols = first_col + lax.broadcasted_iota(jnp.int32, value.shape, 1)
    return jnp.where((rows < size) & (cols < size), value, jnp.zeros_like(value))


def send_body(where, sizes, slots, density, out, targets):
    per_group, slab, width = density.shape
    first = where[0] * per_group
    for slot in range(slots.shape[0]):
        local = slots[slot] - first
        inside = (local >= 0) & (local < per_group)
        targets[jnp.where(inside, local, per_group)] = slot // per_group
    for j in range(per_group):
        rows = masked_rows(
            density[j].astype(F32), sizes[first + j], where[1] * slab, 0
        ).astype(BF16)
        for c in range(width // TILE):
            out[targets[j], c] = rows[:, c * TILE : (c + 1) * TILE]


def tables_body(where, sizes, slots, kind, pack, back):
    groups = back.shape[0] // TILES
    per_group = slots.shape[0] // groups
    first = where[0] * per_group
    widest = jnp.int32(0)
    for group in range(groups):
        total = jnp.int32(0)
        for k in range(per_group):
            total = total + held_slot(sizes, slots, group * per_group, k)[1]
        widest = jnp.maximum(widest, total)
    index = jnp.int32(0)
    for limit in CLASSES[:-1]:
        index = index + (widest > limit).astype(jnp.int32)
    kind[0] = index
    for place in range(pack.shape[0]):
        pack[place] = 0
    for place in range(back.shape[0]):
        back[place] = 0
    offset = jnp.int32(0)
    for k in range(per_group):
        frag, count = held_slot(sizes, slots, first, k)
        source = frag // per_group
        for c in range(TILES):
            valid = c < count
            pack[jnp.where(valid, offset + c, pack.shape[0] - 1)] = source * TILES + c
            back[source * TILES + c] = jnp.where(valid, offset + c, 0)
        offset = offset + count


def fock_body(
    where, sizes, slots, gathered, factors, keep, send, vectors, dense, halved, total, arrived
):
    per_group = factors.shape[0]
    first = where[0] * per_group
    chip = where[3]
    chips, capacity = keep.shape[:2]
    mine = where[2]
    slab = gathered.shape[2]
    chol = factors.shape[1]
    right = (chip + 1) % chips
    left = (chip + chips - 1) % chips
    half = chips // 2

    def copies(k, tiles):
        extent = tiles * TILE
        used = pl.ds(0, extent)
        return [
            pltpu.make_async_copy(
                factors.at[k, q, used, used],
                vectors.at[k, used, pl.ds(q * extent, extent)],
                arrived.at[k, q],
            )
            for q in range(chol)
        ]

    def run(k, offset, tiles):
        extent = tiles * TILE
        bands = extent // slab
        rows = lambda r: pl.ds(r * slab, slab)
        cols = lambda c: slice(c * TILE, (c + 1) * TILE)

        def each(count, step, carry):
            if tiles == TILES:
                return lax.fori_loop(0, count, step, carry)
            for index in range(count):
                carry = step(index, carry)
            return carry

        def unpack(r, carry):
            for c in range(tiles):
                dense[rows(r), cols(c)] = gathered[r, offset + c]
            return carry

        each(bands, unpack, 0)
        for copy in copies(k, tiles):
            copy.wait()
        block = dense[:extent, :extent]
        for q in range(chol):
            span = slice(q * extent, (q + 1) * extent)
            product = jnp.dot(vectors[k, :extent, span], block, preferred_element_type=F32)
            halved[:extent, span] = (-0.5 * product).astype(BF16)
        wide = slice(0, chol * extent)
        total[:extent, :extent] = lax.dot_general(
            halved[:extent, wide],
            vectors[k, :extent, wide],
            (((1,), (1,)), ((), ())),
            preferred_element_type=F32,
        )
        factor = lambda q, r, c: vectors[k, rows(r), cols(q * tiles + c)].astype(F32)

        def weigh(r, sums):
            for c in range(tiles):
                part = dense[rows(r), cols(c)].astype(F32)
                sums = [value + factor(q, r, c) * part for q, value in enumerate(sums)]
            return sums

        sums = each(bands, weigh, [jnp.zeros((slab, TILE), F32) for _ in range(chol)])
        coulomb = [jnp.sum(value, keepdims=True) for value in sums]

        def finish(r, c):
            value = total[rows(r), cols(c)]
            for q in range(chol):
                value = value + coulomb[q] * factor(q, r, c)
            return value

        first_core = mine == 0

        def store(target, carry):
            same = (target + chip) % 2 == 0
            own_row = (target // 2 + half - chip // 2) % half
            up_row = half + (target // 2 + half - right // 2) % half
            down_row = half + (target // 2 + half - left // 2) % half
            for c in range(tiles):
                place = offset + c
                far_row = jnp.where(place < (capacity + 1) // 2, up_row, down_row)
                row = jnp.where(same, own_row, far_row)
                even = finish(2 * target, c)
                odd = finish(2 * target + 1, c)
                keep[row, place] = jnp.where(first_core, even, odd)
                send[row, place] = jnp.where(first_core, odd, even)
            return carry

        each(bands // 2, store, 0)

    for k in range(per_group):
        _, count = held_slot(sizes, slots, first, k)
        for tiles in range(1, TILES + 1):
            pl.when(count == tiles)(lambda: [copy.start() for copy in copies(k, tiles)] and None)

    def slot(k, offset):
        _, count = held_slot(sizes, slots, first, k)
        for tiles in range(1, TILES + 1):
            pl.when(count == tiles)(functools.partial(run, k, offset, tiles))
        return offset + count

    lax.fori_loop(0, per_group, slot, jnp.int32(0))


def base_body(where, sizes, neighbors, low, own, high, hcore, couple, out):
    per_group, slab, _ = own.shape
    first = where[0] * per_group
    row = where[1] * slab
    listed = neighbors.shape[1]

    def fragment(j, carry):
        out[j] = hcore[j].astype(F32)
        for k in range(listed):
            near = neighbors[j, k]
            size = sizes[near]
            weight = couple[j, k].astype(F32)
            place = near - first
            group = jnp.where(place < 0, 0, jnp.where(place < per_group, 1, 2))
            position = place - (group - 1) * per_group

            def add(source):
                rows = masked_rows(source[position].astype(F32), size, row, 0)
                out[j] += weight * rows

            for side, source in enumerate((low, own, high)):
                pl.when(group == side)(functools.partial(add, source))
        return carry

    lax.fori_loop(0, per_group, fragment, 0)


def local(sizes, neighbors, slot_fragment, density, hcore, integrals, couple):
    groups = lax.axis_size("frag")
    cores = lax.axis_size("ka")
    chips = lax.axis_size("tile")
    group = lax.axis_index("frag")
    core = lax.axis_index("ka")
    lane = lax.axis_index("tile") * cores + core
    per_group, slab, width = density.shape
    chol = integrals.shape[1]
    where = jnp.stack([group, lane, core, lax.axis_index("tile")]).astype(jnp.int32)
    shift = lambda value, by: lax.ppermute(
        value, "tile", [(i, (i + by) % chips) for i in range(chips)]
    )

    block = (groups, TILES, slab, TILE)
    table = lambda count: jax.ShapeDtypeStruct((count,), jnp.int32)
    outgoing, targets = pl.pallas_call(
        send_body,
        out_shape=(jax.ShapeDtypeStruct(block, BF16), table(per_group + 1)),
        in_specs=[SMEM, SMEM, SMEM, VMEM],
        out_specs=(VMEM, SMEM),
        compiler_params=pltpu.CompilerParams(vmem_limit_bytes=SMALL_GRANT),
        name="send",
    )(where, sizes, slot_fragment, density)
    received = lax.all_to_all(outgoing, "frag", split_axis=0, concat_axis=0, tiled=True)
    kind, pack, back = pl.pallas_call(
        tables_body,
        out_shape=(table(1), table(per_group * TILES + 1), table(groups * TILES)),
        in_specs=[SMEM] * 3,
        out_specs=(SMEM, SMEM, SMEM),
        name="tables",
    )(where, sizes, slot_fragment)

    def balanced(capacity, received):
        split = (capacity + 1) // 2
        half_chips = chips // 2
        flat = received.reshape(groups * TILES, slab, TILE)
        packed = jnp.take(flat, pack[:capacity], axis=0, mode="clip").astype(F16)
        gathered = lax.all_gather(packed, ("tile", "ka"), axis=0, tiled=False).astype(BF16)
        half = jax.ShapeDtypeStruct((chips, capacity, slab, TILE), F32)
        keep, send = pl.pallas_call(
            fock_body,
            out_shape=(half, half),
            in_specs=[SMEM] * 3 + [VMEM, pl.BlockSpec(memory_space=pl.ANY)],
            out_specs=(VMEM, VMEM),
            scratch_shapes=[
                pltpu.VMEM((per_group, width, chol * width), BF16),
                pltpu.VMEM((width, width), BF16),
                pltpu.VMEM((width, chol * width), BF16),
                pltpu.VMEM((width, width), F32),
                pltpu.SemaphoreType.DMA((per_group, chol)),
            ],
            compiler_params=pltpu.CompilerParams(
                vmem_limit_bytes=(20 + capacity // 2) << 20
            ),
            name="fock",
        )(where, sizes, slot_fragment, gathered, integrals)
        narrow = lambda value: (value * PAIR_SCALE).astype(F16)
        across = lambda value: lax.ppermute(value, "ka", [(0, 1), (1, 0)])
        far = slice(half_chips, chips)
        opposite = (keep[far] * PAIR_SCALE + across(narrow(send[far])).astype(F32)).astype(F16)
        up = shift(opposite[:, :split], 1)
        down = shift(opposite[:, split:], -1)
        low = lax.ppermute(density, "frag", [(i, i + 1) for i in range(groups - 1)])
        high = lax.ppermute(density, "frag", [(i + 1, i) for i in range(groups - 1)])
        near = slice(0, half_chips)
        pair = keep[near] * PAIR_SCALE + across(narrow(send[near])).astype(F32)
        own = pair + jnp.concatenate([up, down], axis=1).astype(F32)
        moved = [shift(own[step].astype(F16), 2 * step) for step in range(1, half_chips)]
        total = own[0] + sum(part.astype(F32) for part in moved)
        total = lax.optimization_barrier((total * (SUM_SCALE / PAIR_SCALE)).astype(F16))
        return jnp.take(total, back, axis=0, mode="clip"), low, high

    branches = [functools.partial(balanced, capacity) for capacity in CLASSES]
    summed, low, high = lax.switch(kind[0], branches, received)
    summed = summed.reshape(block)
    returned = lax.all_to_all(summed, "frag", split_axis=0, concat_axis=0, tiled=True)
    base = pl.pallas_call(
        base_body,
        out_shape=jax.ShapeDtypeStruct(density.shape, F32),
        in_specs=[SMEM] * 3 + [VMEM] * 5,
        out_specs=VMEM,
        compiler_params=pltpu.CompilerParams(vmem_limit_bytes=SMALL_GRANT),
        name="base",
    )(where, sizes, neighbors, low, density, high, hcore, couple)
    picked = jnp.take(returned, targets[:per_group], axis=0, mode="clip")
    two_body = picked.astype(F32).transpose(0, 2, 1, 3).reshape(density.shape)
    own_sizes = lax.dynamic_slice_in_dim(sizes, group * per_group, per_group)[:, None, None]
    rows = lane * slab + lax.broadcasted_iota(jnp.int32, density.shape, 1)
    cols = lax.broadcasted_iota(jnp.int32, density.shape, 2)
    keep = (rows < own_sizes) & (cols < own_sizes)
    return jnp.where(keep, base + two_body * (1.0 / SUM_SCALE), 0.0)


def solution(mesh):
    return jax.shard_map(
        local,
        mesh=mesh,
        in_specs=(
            P(),
            P("frag", None),
            P(),
            P("frag", ("tile", "ka"), None),
            P("frag", ("tile", "ka"), None),
            P("frag", ("tile", "ka"), None, None),
            P("frag", None, ("tile", "ka"), None),
        ),
        out_specs=P("frag", ("tile", "ka"), None),
        check_vma=False,
    )
```

```python
import functools

import jax
import jax.numpy as jnp
from jax import lax
from jax.experimental import pallas as pl
from jax.experimental.pallas import tpu as pltpu
from jax.sharding import PartitionSpec as P


F16 = jnp.float16
F32 = jnp.float32
BF16 = jnp.bfloat16
TILE = 128
TILES = 4
CLASSES = (16, 18, 21, 32)
PAIR_SCALE = 0.25
SUM_SCALE = 0.03125
SMALL_GRANT = 8 << 20
SMEM = pl.BlockSpec(memory_space=pltpu.SMEM)
VMEM = pl.BlockSpec(memory_space=pltpu.VMEM)


def tiles_of(size):
    return (size + (TILE - 1)) // TILE


def held_slot(sizes, slots, first, k):
    frag = slots[first + k]
    return frag, tiles_of(sizes[frag])


def masked_rows(value, size, first_row, first_col):
    rows = first_row + lax.broadcasted_iota(jnp.int32, value.shape, 0)
    cols = first_col + lax.broadcasted_iota(jnp.int32, value.shape, 1)
    return jnp.where((rows < size) & (cols < size), value, jnp.zeros_like(value))


def send_body(where, sizes, slots, density, out, targets):
    per_group, slab, width = density.shape
    first = where[0] * per_group
    for slot in range(slots.shape[0]):
        local = slots[slot] - first
        inside = (local >= 0) & (local < per_group)
        targets[jnp.where(inside, local, per_group)] = slot // per_group
    for j in range(per_group):
        rows = masked_rows(
            density[j].astype(F32), sizes[first + j], where[1] * slab, 0
        ).astype(BF16)
        for c in range(width // TILE):
            out[targets[j], c] = rows[:, c * TILE : (c + 1) * TILE]


def tables_body(where, sizes, slots, kind, pack, back):
    groups = back.shape[0] // TILES
    per_group = slots.shape[0] // groups
    first = where[0] * per_group
    widest = jnp.int32(0)
    for group in range(groups):
        total = jnp.int32(0)
        for k in range(per_group):
            total = total + held_slot(sizes, slots, group * per_group, k)[1]
        widest = jnp.maximum(widest, total)
    index = jnp.int32(0)
    for limit in CLASSES[:-1]:
        index = index + (widest > limit).astype(jnp.int32)
    kind[0] = index
    for place in range(pack.shape[0]):
        pack[place] = 0
    for place in range(back.shape[0]):
        back[place] = 0
    offset = jnp.int32(0)
    for k in range(per_group):
        frag, count = held_slot(sizes, slots, first, k)
        source = frag // per_group
        for c in range(TILES):
            valid = c < count
            pack[jnp.where(valid, offset + c, pack.shape[0] - 1)] = source * TILES + c
            back[source * TILES + c] = jnp.where(valid, offset + c, 0)
        offset = offset + count


def fock_body(
    where, sizes, slots, gathered, factors, keep, send, vectors, dense, halved, total, arrived
):
    per_group = factors.shape[0]
    first = where[0] * per_group
    chip = where[3]
    chips, capacity = keep.shape[:2]
    mine = where[2]
    slab = gathered.shape[2]
    chol = factors.shape[1]
    right = (chip + 1) % chips
    left = (chip + chips - 1) % chips
    half = chips // 2

    def copies(k, tiles):
        extent = tiles * TILE
        used = pl.ds(0, extent)
        return [
            pltpu.make_async_copy(
                factors.at[k, q, used, used],
                vectors.at[k, used, pl.ds(q * extent, extent)],
                arrived.at[k, q],
            )
            for q in range(chol)
        ]

    def run(k, offset, tiles):
        extent = tiles * TILE
        bands = extent // slab
        rows = lambda r: pl.ds(r * slab, slab)
        cols = lambda c: slice(c * TILE, (c + 1) * TILE)

        def each(count, step, carry):
            if tiles == TILES:
                return lax.fori_loop(0, count, step, carry)
            for index in range(count):
                carry = step(index, carry)
            return carry

        def unpack(r, carry):
            for c in range(tiles):
                dense[rows(r), cols(c)] = gathered[r, offset + c]
            return carry

        each(bands, unpack, 0)
        for copy in copies(k, tiles):
            copy.wait()
        block = dense[:extent, :extent]
        for q in range(chol):
            span = slice(q * extent, (q + 1) * extent)
            product = jnp.dot(vectors[k, :extent, span], block, preferred_element_type=F32)
            halved[:extent, span] = (-0.5 * product).astype(BF16)
        wide = slice(0, chol * extent)
        total[:extent, :extent] = lax.dot_general(
            halved[:extent, wide],
            vectors[k, :extent, wide],
            (((1,), (1,)), ((), ())),
            preferred_element_type=F32,
        )
        factor = lambda q, r, c: vectors[k, rows(r), cols(q * tiles + c)].astype(F32)

        def weigh(r, sums):
            for c in range(tiles):
                part = dense[rows(r), cols(c)].astype(F32)
                sums = [value + factor(q, r, c) * part for q, value in enumerate(sums)]
            return sums

        sums = each(bands, weigh, [jnp.zeros((slab, TILE), F32) for _ in range(chol)])
        coulomb = [jnp.sum(value, keepdims=True) for value in sums]

        def finish(r, c):
            value = total[rows(r), cols(c)]
            for q in range(chol):
                value = value + coulomb[q] * factor(q, r, c)
            return value

        first_core = mine == 0

        def store(target, carry):
            same = (target + chip) % 2 == 0
            own_row = (target // 2 + half - chip // 2) % half
            up_row = half + (target // 2 + half - right // 2) % half
            down_row = half + (target // 2 + half - left // 2) % half
            for c in range(tiles):
                place = offset + c
                far_row = jnp.where(place < (capacity + 1) // 2, up_row, down_row)
                row = jnp.where(same, own_row, far_row)
                even = finish(2 * target, c)
                odd = finish(2 * target + 1, c)
                keep[row, place] = jnp.where(first_core, even, odd)
                send[row, place] = jnp.where(first_core, odd, even)
            return carry

        each(bands // 2, store, 0)

    for k in range(per_group):
        _, count = held_slot(sizes, slots, first, k)
        for tiles in range(1, TILES + 1):
            pl.when(count == tiles)(lambda: [copy.start() for copy in copies(k, tiles)] and None)

    def slot(k, offset):
        _, count = held_slot(sizes, slots, first, k)
        for tiles in range(1, TILES + 1):
            pl.when(count == tiles)(functools.partial(run, k, offset, tiles))
        return offset + count

    lax.fori_loop(0, per_group, slot, jnp.int32(0))


def base_body(where, sizes, neighbors, low, own, high, hcore, couple, out):
    per_group, slab, _ = own.shape
    first = where[0] * per_group
    row = where[1] * slab
    listed = neighbors.shape[1]

    def fragment(j, carry):
        out[j] = hcore[j].astype(F32)
        for k in range(listed):
            near = neighbors[j, k]
            size = sizes[near]
            weight = couple[j, k].astype(F32)
            place = near - first
            group = jnp.where(place < 0, 0, jnp.where(place < per_group, 1, 2))
            position = place - (group - 1) * per_group

            def add(source):
                rows = masked_rows(source[position].astype(F32), size, row, 0)
                out[j] += weight * rows

            for side, source in enumerate((low, own, high)):
                pl.when(group == side)(functools.partial(add, source))
        return carry

    lax.fori_loop(0, per_group, fragment, 0)


def local(sizes, neighbors, slot_fragment, density, hcore, integrals, couple):
    groups = lax.axis_size("frag")
    cores = lax.axis_size("ka")
    chips = lax.axis_size("tile")
    group = lax.axis_index("frag")
    core = lax.axis_index("ka")
    lane = lax.axis_index("tile") * cores + core
    per_group, slab, width = density.shape
    chol = integrals.shape[1]
    where = jnp.stack([group, lane, core, lax.axis_index("tile")]).astype(jnp.int32)
    shift = lambda value, by: lax.ppermute(
        value, "tile", [(i, (i + by) % chips) for i in range(chips)]
    )

    block = (groups, TILES, slab, TILE)
    table = lambda count: jax.ShapeDtypeStruct((count,), jnp.int32)
    outgoing, targets = pl.pallas_call(
        send_body,
        out_shape=(jax.ShapeDtypeStruct(block, BF16), table(per_group + 1)),
        in_specs=[SMEM, SMEM, SMEM, VMEM],
        out_specs=(VMEM, SMEM),
        compiler_params=pltpu.CompilerParams(vmem_limit_bytes=SMALL_GRANT),
        name="send",
    )(where, sizes, slot_fragment, density)
    received = lax.all_to_all(outgoing, "frag", split_axis=0, concat_axis=0, tiled=True)
    kind, pack, back = pl.pallas_call(
        tables_body,
        out_shape=(table(1), table(per_group * TILES + 1), table(groups * TILES)),
        in_specs=[SMEM] * 3,
        out_specs=(SMEM, SMEM, SMEM),
        name="tables",
    )(where, sizes, slot_fragment)

    def balanced(capacity, received):
        split = (capacity + 1) // 2
        half_chips = chips // 2
        flat = received.reshape(groups * TILES, slab, TILE)
        packed = jnp.take(flat, pack[:capacity], axis=0, mode="clip").astype(F16)
        gathered = lax.all_gather(packed, ("tile", "ka"), axis=0, tiled=False).astype(BF16)
        half = jax.ShapeDtypeStruct((chips, capacity, slab, TILE), F32)
        keep, send = pl.pallas_call(
            fock_body,
            out_shape=(half, half),
            in_specs=[SMEM] * 3 + [VMEM, pl.BlockSpec(memory_space=pl.ANY)],
            out_specs=(VMEM, VMEM),
            scratch_shapes=[
                pltpu.VMEM((per_group, width, chol * width), BF16),
                pltpu.VMEM((width, width), BF16),
                pltpu.VMEM((width, chol * width), BF16),
                pltpu.VMEM((width, width), F32),
                pltpu.SemaphoreType.DMA((per_group, chol)),
            ],
            compiler_params=pltpu.CompilerParams(
                vmem_limit_bytes=(20 + capacity // 2) << 20
            ),
            name="fock",
        )(where, sizes, slot_fragment, gathered, integrals)
        narrow = lambda value: (value * PAIR_SCALE).astype(F16)
        across = lambda value: lax.ppermute(value, "ka", [(0, 1), (1, 0)])
        far = slice(half_chips, chips)
        opposite = (keep[far] * PAIR_SCALE + across(narrow(send[far])).astype(F32)).astype(F16)
        up = shift(opposite[:, :split], 1)
        down = shift(opposite[:, split:], -1)
        low = lax.ppermute(density, "frag", [(i, i + 1) for i in range(groups - 1)])
        high = lax.ppermute(density, "frag", [(i + 1, i) for i in range(groups - 1)])
        near = slice(0, half_chips)
        pair = keep[near] * PAIR_SCALE + across(narrow(send[near])).astype(F32)
        own = pair + jnp.concatenate([up, down], axis=1).astype(F32)
        middle = half_chips // 2
        moved = [shift(own[middle].astype(F16), 2 * middle)]
        moved += [
            shift(own[step].astype(F16), 2 * step)
            for step in range(1, half_chips)
            if step != middle
        ]
        total = own[0] + sum(part.astype(F32) for part in moved)
        total = lax.optimization_barrier((total * (SUM_SCALE / PAIR_SCALE)).astype(F16))
        return jnp.take(total, back, axis=0, mode="clip"), low, high

    branches = [functools.partial(balanced, capacity) for capacity in CLASSES]
    summed, low, high = lax.switch(kind[0], branches, received)
    summed = summed.reshape(block)
    returned = lax.all_to_all(summed, "frag", split_axis=0, concat_axis=0, tiled=True)
    base = pl.pallas_call(
        base_body,
        out_shape=jax.ShapeDtypeStruct(density.shape, F32),
        in_specs=[SMEM] * 3 + [VMEM] * 5,
        out_specs=VMEM,
        compiler_params=pltpu.CompilerParams(vmem_limit_bytes=SMALL_GRANT),
        name="base",
    )(where, sizes, neighbors, low, density, high, hcore, couple)
    picked = jnp.take(returned, targets[:per_group], axis=0, mode="clip")
    two_body = picked.astype(F32).transpose(0, 2, 1, 3).reshape(density.shape)
    own_sizes = lax.dynamic_slice_in_dim(sizes, group * per_group, per_group)[:, None, None]
    rows = lane * slab + lax.broadcasted_iota(jnp.int32, density.shape, 1)
    cols = lax.broadcasted_iota(jnp.int32, density.shape, 2)
    keep = (rows < own_sizes) & (cols < own_sizes)
    return jnp.where(keep, base + two_body * (1.0 / SUM_SCALE), 0.0)


def solution(mesh):
    return jax.shard_map(
        local,
        mesh=mesh,
        in_specs=(
            P(),
            P("frag", None),
            P(),
            P("frag", ("tile", "ka"), None),
            P("frag", ("tile", "ka"), None),
            P("frag", ("tile", "ka"), None, None),
            P("frag", None, ("tile", "ka"), None),
        ),
        out_specs=P("frag", ("tile", "ka"), None),
        check_vma=False,
    )
```
